32 devices in a mesh: ta: 16 (over z, x, core), aa: 2 (over y).
Axes of the slice: x: 2, y: 2, z: 4, core: 2. Of those that a mesh axis runs over, the one named last changes fastest.
Arguments:
- voltages: bfloat16 [256, 393216], P('aa', 'ta'), may hold values from -6 to 6
- pfb_window: float32 [4, 8192], replicated, may hold values from -3 to 3
Outputs:
- visibilities: float32 [2048, 256, 512], P('ta', 'aa')
The draws below stay inside these ranges and needn't reach their ends.
All inputs are finite; a program needn't handle non-finite values.
Results may differ from the reference program's by a relative error of at most 0.0026.
Values may be sent and summed in bfloat16 or wider, within the bound.
A program may use at most 192 MiB of HBM per device.

```python
import math
import jax
import jax.numpy as jnp
from jax import lax

S = 256
NFFT = 8192
CH = 2048
TAPS = 4
FRAMES = 48
CH_OFF = 1024


def steps_of(rng, dims, pieces, least, high):
    gain = 1.0
    for axis_at, blocks in pieces:
        heights = jax.random.uniform(jax.random.fold_in(jax.random.fold_in(rng, 6), axis_at), (blocks,), jnp.float32, least / len(pieces), high / len(pieces))
        gain = gain * jnp.repeat(jnp.exp(heights), dims[axis_at] // blocks).reshape((-1,) + (1,) * (len(dims) - 1 - axis_at))
    return gain


def scatter_about(key, dims, scale, bound, cuts=(), held_as=jnp.bfloat16):
    values = scale * jax.random.normal(key, dims, jnp.float32)
    if cuts:
        values = values * steps_of(key, dims, cuts, -0.22, 0.18)
    return jnp.clip(values, -bound, bound).astype(held_as)


def setup_inputs(seed: int = 0) -> dict:
    streams_of = jax.random.split(jax.random.key(seed), 3)
    return {
        "voltages": scatter_about(streams_of[0], (S, FRAMES * NFFT), 1.0, 6.0, ((0, 2), (1, 16))),
        "pfb_window": scatter_about(streams_of[1], (TAPS, NFFT), 0.5, 3.0, (), jnp.float32),
    }


def reference(voltages, pfb_window):
    frames = voltages.shape[1] // NFFT
    padded = jnp.concatenate([jnp.zeros((S, (TAPS - 1) * NFFT), voltages.dtype), voltages], axis=1)
    window = pfb_window.astype(jnp.float32)

    def one_frame(frame_index):
        start_index = (frame_index * NFFT).astype(jnp.int32)
        samples = lax.dynamic_slice_in_dim(padded, start_index, TAPS * NFFT, 1)
        samples = samples.astype(jnp.float32).reshape(S, TAPS, NFFT)
        filtered = lax.optimization_barrier(jnp.sum(samples * window[None], axis=1))
        spectrum = jnp.fft.rfft(filtered, axis=1)[:, CH_OFF:CH_OFF + CH] / math.sqrt(NFFT)
        stacked = jnp.stack([jnp.real(spectrum), jnp.imag(spectrum)], axis=0).astype(jnp.float32)
        return jnp.transpose(stacked, (2, 0, 1)).astype(jnp.bfloat16)
    spectra = lax.map(one_frame, jnp.arange(frames, dtype=jnp.int32))
    spectra = jnp.transpose(spectra, (1, 0, 2, 3))
    scaling = 1.0 / math.sqrt(frames)
    blocks = spectra.reshape(CH // 16, 16, frames, 2, S)

    def one_block(channel_block):
        values = channel_block.astype(jnp.float32)
        swapped = jnp.stack([values[:, :, 1], -values[:, :, 0]], axis=2)
        left_rows = jnp.concatenate([values, swapped], axis=3)
        result = jnp.einsum('cfpi,cfpj->cij', left_rows, values) * scaling
        return jnp.concatenate([result[:, :S], result[:, S:]], axis=2)
    visible = lax.map(one_block, blocks)
    return visible.reshape(CH, S, 2 * S)
```

```python
import functools
import math

import jax
import jax.numpy as jnp
import numpy as np
from jax import lax
from jax.experimental import pallas as pl
from jax.experimental.pallas import tpu as pltpu
from jax.sharding import PartitionSpec as P

NFFT = 8192
CH = 2048
TAPS = 4
CH_OFF = 1024
RADIX = 32
INNER = NFFT // RADIX
BINS = CH // RADIX
HALF = RADIX // 2
LANES = 128
SIG_BLOCK = 16


def split_bf16(x):
    hi = jnp.asarray(x, jnp.bfloat16)
    return hi, (x - hi.astype(jnp.float32)).astype(jnp.bfloat16)


def stage_two_matrix():
    n2 = np.arange(INNER)[None, :]
    m = np.arange(BINS)[:, None] + CH_OFF // RADIX
    angle = 2.0 * np.pi * ((n2 * m) % INNER) / INNER
    mirror = 2.0 * np.pi * ((n2 * (m + 1)) % INNER) / INNER
    rows = [
        np.concatenate([np.cos(angle), np.sin(angle)], axis=1),
        np.concatenate([-np.sin(angle), np.cos(angle)], axis=1),
        np.concatenate([np.cos(mirror), -np.sin(mirror)], axis=1),
        np.concatenate([-np.sin(mirror), -np.cos(mirror)], axis=1),
    ]
    full = np.concatenate(rows, axis=0) / math.sqrt(NFFT)
    hi = full.astype(jnp.bfloat16)
    lo = (full - hi.astype(np.float64)).astype(jnp.bfloat16)
    return hi, lo


def twist_table():
    k = np.arange(HALF + 1)[:, None]
    n2 = np.arange(INNER)[None, :]
    angle = 2.0 * np.pi * (k * n2) / NFFT
    return np.stack([np.cos(angle), -np.sin(angle)]).astype(np.float32)


def rfft_list(x):
    n = len(x)
    if n == 2:
        return [(x[0] + x[1], None), (x[0] - x[1], None)]
    even, odd = rfft_list(x[0::2]), rfft_list(x[1::2])
    out = [None] * (n // 2 + 1)
    for k in range(n // 4 + 1):
        er, ei = even[k]
        our, oui = odd[k]
        if k == 0:
            out[0] = (er + our, None)
            out[n // 2] = (er - our, None)
        elif k == n // 4:
            out[k] = (er, -our)
        else:
            c = math.cos(2 * math.pi * k / n)
            s = math.sin(2 * math.pi * k / n)
            if 8 * k == n:
                tr, ti = (our + oui) * c, (oui - our) * c
            else:
                tr, ti = our * c + oui * s, oui * c - our * s
            out[k] = (er + tr, ei + ti)
            out[n // 2 - k] = (er - tr, ti - ei)
    return out


def channel_kernel(steps, signals, *refs):
    taps = refs[:TAPS]
    win, twist, mat_hi, mat_lo, out, hi_s, lo_s, spec_s = refs[TAPS:]
    step = pl.program_id(0)
    rows = pl.ds(pl.multiple_of(step * SIG_BLOCK, SIG_BLOCK), SIG_BLOCK)

    for part in range(INNER // LANES):
        filtered = []
        for n1 in range(RADIX):
            cols = pl.ds(n1 * INNER + part * LANES, LANES)
            total = win[0:1, cols] * taps[0][:, cols].astype(jnp.float32)
            for t in range(1, TAPS):
                total = total + win[t : t + 1, cols] * taps[t][:, cols].astype(jnp.float32)
            filtered.append(total)
        here = pl.ds(part * LANES, LANES)
        there = pl.ds(INNER + part * LANES, LANES)
        for k, (ar, ai) in enumerate(rfft_list(filtered)):
            if k == 0:
                br, bi = ar, jnp.zeros_like(ar)
            else:
                tr, ti = twist[0, k : k + 1, here], twist[1, k : k + 1, here]
                if ai is None:
                    br, bi = ar * tr, ar * ti
                else:
                    br, bi = ar * tr - ai * ti, ar * ti + ai * tr
            for value, cols in ((br, here), (bi, there)):
                hi, lo = split_bf16(value)
                hi_s[k, rows, cols] = hi
                lo_s[k, rows, cols] = lo

    @pl.when(step == steps - 1)
    def _():
        dims = (((1,), (1,)), ((), ()))

        def dot(a, b):
            return lax.dot_general(a, b, dims, preferred_element_type=jnp.float32)

        def put(value, k):
            spec_s[0, pl.ds(k, BINS, stride=RADIX), :] = value[:BINS]
            spec_s[1, pl.ds(k, BINS, stride=RADIX), :] = value[BINS:]

        for k in range(HALF + 1):
            size = 2 * BINS if k in (0, HALF) else 4 * BINS
            a_hi, a_lo = mat_hi[:size, :], mat_lo[:size, :]
            b_hi, b_lo = hi_s[k], lo_s[k]
            res = dot(a_hi, b_hi) + (dot(a_hi, b_lo) + dot(a_lo, b_hi))
            put(res[: 2 * BINS], k)
            if size > 2 * BINS:
                put(res[2 * BINS :], RADIX - k)

        def cast(i, carry):
            at = pl.ds(pl.multiple_of(i * 64, 64), 64)
            out[at, :signals] = spec_s[0, at, :].astype(jnp.bfloat16)
            out[at, signals:] = spec_s[1, at, :].astype(jnp.bfloat16)
            return carry

        lax.fori_loop(0, CH // 64, cast, 0)


def channelize(pieces, window, signals):
    steps = signals // SIG_BLOCK
    mat_hi, mat_lo = stage_two_matrix()

    def tap_spec(frame):
        return pl.BlockSpec((SIG_BLOCK, NFFT), lambda i, frame=frame: (i, frame))

    whole = lambda shape: pl.BlockSpec(shape, lambda i: (0,) * len(shape))
    return pl.pallas_call(
        functools.partial(channel_kernel, steps, signals),
        grid=(steps,),
        out_shape=jax.ShapeDtypeStruct((CH, 2 * signals), jnp.bfloat16),
        in_specs=[tap_spec(frame) for _, frame in pieces]
        + [
            whole((TAPS, NFFT)),
            whole((2, HALF + 1, INNER)),
            whole((4 * BINS, 2 * INNER)),
            whole((4 * BINS, 2 * INNER)),
        ],
        out_specs=whole((CH, 2 * signals)),
        scratch_shapes=[
            pltpu.VMEM((HALF + 1, signals, 2 * INNER), jnp.bfloat16),
            pltpu.VMEM((HALF + 1, signals, 2 * INNER), jnp.bfloat16),
            pltpu.VMEM((2, CH, signals), jnp.float32),
        ],
        compiler_params=pltpu.CompilerParams(
            dimension_semantics=("arbitrary",), vmem_limit_bytes=48 * 1024 * 1024
        ),
        cost_estimate=pl.CostEstimate(
            flops=8_000_000_000, bytes_accessed=10_000_000, transcendentals=0
        ),
    )(
        *[piece for piece, _ in pieces],
        window,
        jnp.asarray(twist_table()),
        jnp.asarray(mat_hi),
        jnp.asarray(mat_lo),
    )


def correlate_kernel(chunks, signals, block, scale, *refs):
    position = lax.rem(refs[0][0], 2)
    own = refs[1 : 1 + chunks]
    other = refs[1 + chunks : 1 + 2 * chunks]
    out = refs[-1]
    dims = (((0,), (0,)), ((), ()))
    for c in range(block):
        xr = [r[c, :, :signals] for r in own]
        xi = [r[c, :, signals:] for r in own]
        left = jnp.concatenate(xr + xi, axis=0)
        turned = jnp.concatenate([-v for v in xi] + xr, axis=0)
        yr = [r[c, :, :signals] for r in other]
        yi = [r[c, :, signals:] for r in other]
        far = jnp.concatenate(yr + yi, axis=0)
        far_turned = jnp.concatenate([-v for v in yi] + yr, axis=0)
        near = lax.dot_general(
            left, jnp.concatenate([left, turned], axis=1), dims,
            preferred_element_type=jnp.float32) * scale
        away = lax.dot_general(
            left, jnp.concatenate([far, far_turned], axis=1), dims,
            preferred_element_type=jnp.float32) * scale
        for half in range(2):
            lanes = slice(half * signals, (half + 1) * signals)
            base = half * 2 * signals
            first = pl.multiple_of(base + position * signals, signals)
            second = pl.multiple_of(base + (1 - position) * signals, signals)
            out[c, :, pl.ds(first, signals)] = near[:, lanes]
            out[c, :, pl.ds(second, signals)] = away[:, lanes]


def correlate(own, other, scale, signals):
    channels, peers, _ = own[0].shape
    block = 8
    spec = pl.BlockSpec((block, peers, 2 * signals), lambda i, *_: (i, 0, 0))
    return pl.pallas_call(
        functools.partial(correlate_kernel, len(own), signals, block, scale),
        grid_spec=pltpu.PrefetchScalarGridSpec(
            num_scalar_prefetch=1,
            grid=(channels // block,),
            in_specs=[spec] * (2 * len(own)),
            out_specs=pl.BlockSpec((block, signals, 4 * signals), lambda i, *_: (i, 0, 0)),
        ),
        out_shape=jax.ShapeDtypeStruct((channels, signals, 4 * signals), jnp.float32),
        compiler_params=pltpu.CompilerParams(
            dimension_semantics=("arbitrary",), vmem_limit_bytes=48 * 1024 * 1024
        ),
        cost_estimate=pl.CostEstimate(
            flops=3_000_000_000, bytes_accessed=40_000_000, transcendentals=0
        ),
    )(lax.axis_index("aa").astype(jnp.int32).reshape(1), *own, *other)


def per_device(voltages, pfb_window):
    signals, samples = voltages.shape
    frames = samples // NFFT
    peers = lax.axis_size("ta")
    sides = lax.axis_size("aa")
    assert sides == 2 and frames >= TAPS - 1 and signals % LANES == 0
    onward = [(i, i + 1) for i in range(peers - 1)]
    across = [(i, 1 - i) for i in range(sides)]

    history = {}
    for frame in range(frames - 1, frames - TAPS, -1):
        tail = voltages[:, frame * NFFT : (frame + 1) * NFFT]
        history[frame - frames] = lax.ppermute(tail, "ta", onward)

    own, other = [], []
    for frame in range(frames - 1, -1, -1):
        pieces = []
        for tap in range(TAPS):
            at = frame - (TAPS - 1) + tap
            pieces.append((voltages, at) if at >= 0 else (history[at], 0))
        spectra = channelize(pieces, pfb_window, signals)
        owned = lax.all_to_all(
            spectra.reshape(peers, CH // peers, 2 * signals), "ta",
            split_axis=0, concat_axis=0, tiled=True)
        owned = jnp.transpose(owned, (1, 0, 2))
        own.append(owned)
        other.append(lax.ppermute(owned, "aa", across))
    scale = 1.0 / math.sqrt(frames * peers)
    return correlate(own, other, scale, signals)


def solution(mesh):
    in_specs = (P("aa", "ta"), P())
    out_specs = P("ta", "aa", None)
    return jax.shard_map(
        per_device, mesh=mesh, in_specs=in_specs, out_specs=out_specs, check_vma=False
    )
```

```python
import functools
import math

import jax
import jax.numpy as jnp
import numpy as np
from jax import lax
from jax.experimental import pallas as pl
from jax.experimental.pallas import tpu as pltpu
from jax.sharding import PartitionSpec as P


NFFT = 8192
CH = 2048
TAPS = 4
CH_OFF = 1024
RADIX = 32
INNER = NFFT // RADIX
BINS = CH // RADIX
HALF = RADIX // 2
LANES = 128
SIG_BLOCK = 16


def split_bf16(x):
    hi = jnp.asarray(x, jnp.bfloat16)
    return hi, (x - hi.astype(jnp.float32)).astype(jnp.bfloat16)


def stage_two_matrix():
    n2 = np.arange(INNER)[None, :]
    m = np.arange(BINS)[:, None] + CH_OFF // RADIX
    angle = 2.0 * np.pi * ((n2 * m) % INNER) / INNER
    mirror = 2.0 * np.pi * ((n2 * (m + 1)) % INNER) / INNER
    rows = [
        np.concatenate([np.cos(angle), np.sin(angle)], axis=1),
        np.concatenate([-np.sin(angle), np.cos(angle)], axis=1),
        np.concatenate([np.cos(mirror), -np.sin(mirror)], axis=1),
        np.concatenate([-np.sin(mirror), -np.cos(mirror)], axis=1),
    ]
    full = np.concatenate(rows, axis=0) / math.sqrt(NFFT)
    hi = full.astype(jnp.bfloat16)
    lo = (full - hi.astype(np.float64)).astype(jnp.bfloat16)
    return hi, lo


def twist_table():
    k = np.arange(HALF + 1)[:, None]
    n2 = np.arange(INNER)[None, :]
    angle = 2.0 * np.pi * (k * n2) / NFFT
    return np.stack([np.cos(angle), -np.sin(angle)]).astype(np.float32)


def rfft_list(x):
    n = len(x)
    if n == 2:
        return [(x[0] + x[1], None), (x[0] - x[1], None)]
    even, odd = rfft_list(x[0::2]), rfft_list(x[1::2])
    out = [None] * (n // 2 + 1)
    for k in range(n // 4 + 1):
        er, ei = even[k]
        our, oui = odd[k]
        if k == 0:
            out[0] = (er + our, None)
            out[n // 2] = (er - our, None)
        elif k == n // 4:
            out[k] = (er, -our)
        else:
            c = math.cos(2 * math.pi * k / n)
            s = math.sin(2 * math.pi * k / n)
            if 8 * k == n:
                tr, ti = (our + oui) * c, (oui - our) * c
            else:
                tr, ti = our * c + oui * s, oui * c - our * s
            out[k] = (er + tr, ei + ti)
            out[n // 2 - k] = (er - tr, ti - ei)
    return out


def channel_kernel(steps, signals, *refs):
    taps = refs[:TAPS]
    win, twist, mat_hi, mat_lo, out, parts_s, spec_s = refs[TAPS:]
    step = pl.program_id(0)
    rows = pl.ds(pl.multiple_of(step * SIG_BLOCK, SIG_BLOCK), SIG_BLOCK)
    low_rows = pl.ds(pl.multiple_of(signals + step * SIG_BLOCK, SIG_BLOCK), SIG_BLOCK)

    for part in range(INNER // LANES):
        filtered = []
        for n1 in range(RADIX):
            cols = pl.ds(n1 * INNER + part * LANES, LANES)
            total = win[0:1, cols] * taps[0][:, cols].astype(jnp.float32)
            for t in range(1, TAPS):
                total = total + win[t : t + 1, cols] * taps[t][:, cols].astype(jnp.float32)
            filtered.append(total)
        here = pl.ds(part * LANES, LANES)
        there = pl.ds(INNER + part * LANES, LANES)
        for k, (ar, ai) in enumerate(rfft_list(filtered)):
            if k == 0:
                br, bi = ar, jnp.zeros_like(ar)
            else:
                tr, ti = twist[0, k : k + 1, here], twist[1, k : k + 1, here]
                if ai is None:
                    br, bi = ar * tr, ar * ti
                else:
                    br, bi = ar * tr - ai * ti, ar * ti + ai * tr
            for value, cols in ((br, here), (bi, there)):
                hi, lo = split_bf16(value)
                parts_s[k, rows, cols] = hi
                parts_s[k, low_rows, cols] = lo

    @pl.when(step == steps - 1)
    def _():
        dims = (((1,), (1,)), ((), ()))

        def dot(a, b):
            return lax.dot_general(a, b, dims, preferred_element_type=jnp.float32)

        def put(value, k):
            spec_s[0, pl.ds(k, BINS, stride=RADIX), :] = value[:BINS]
            spec_s[1, pl.ds(k, BINS, stride=RADIX), :] = value[BINS:]

        for k in range(HALF + 1):
            size = 2 * BINS if k in (0, HALF) else 4 * BINS
            a_hi, a_lo = mat_hi[:size, :], mat_lo[:size, :]
            both = dot(a_hi, parts_s[k])
            small = dot(a_lo, parts_s[k, :signals])
            res = both[:, :signals] + (both[:, signals:] + small)
            put(res[: 2 * BINS], k)
            if size > 2 * BINS:
                put(res[2 * BINS :], RADIX - k)

        def cast(i, carry):
            at = pl.ds(pl.multiple_of(i * 64, 64), 64)
            out[at, :signals] = spec_s[0, at, :].astype(jnp.bfloat16)
            out[at, signals:] = spec_s[1, at, :].astype(jnp.bfloat16)
            return carry

        lax.fori_loop(0, CH // 64, cast, 0)


def channelize(pieces, window, signals):
    steps = signals // SIG_BLOCK
    mat_hi, mat_lo = stage_two_matrix()

    def tap_spec(frame):
        return pl.BlockSpec((SIG_BLOCK, NFFT), lambda i, frame=frame: (i, frame))

    whole = lambda shape: pl.BlockSpec(shape, lambda i: (0,) * len(shape))
    return pl.pallas_call(
        functools.partial(channel_kernel, steps, signals),
        grid=(steps,),
        out_shape=jax.ShapeDtypeStruct((CH, 2 * signals), jnp.bfloat16),
        in_specs=[tap_spec(frame) for _, frame in pieces]
        + [
            whole((TAPS, NFFT)),
            whole((2, HALF + 1, INNER)),
            whole((4 * BINS, 2 * INNER)),
            whole((4 * BINS, 2 * INNER)),
        ],
        out_specs=whole((CH, 2 * signals)),
        scratch_shapes=[
            pltpu.VMEM((HALF + 1, 2 * signals, 2 * INNER), jnp.bfloat16),
            pltpu.VMEM((2, CH, signals), jnp.float32),
        ],
        compiler_params=pltpu.CompilerParams(
            dimension_semantics=("arbitrary",), vmem_limit_bytes=48 * 1024 * 1024
        ),
        cost_estimate=pl.CostEstimate(
            flops=8_000_000_000, bytes_accessed=10_000_000, transcendentals=0
        ),
    )(
        *[piece for piece, _ in pieces],
        window,
        jnp.asarray(twist_table()),
        jnp.asarray(mat_hi),
        jnp.asarray(mat_lo),
    )


def correlate_kernel(chunks, signals, block, scale, *refs):
    mine = refs[1 : 1 + chunks]
    far = refs[1 + chunks : 1 + 2 * chunks]
    out = refs[-1]
    dims = (((0,), (0,)), ((), ()))

    def write(right_of):
        for c in range(block):
            left = [r[c, :, :signals] for r in mine] + [r[c, :, signals:] for r in mine]
            out[c] = lax.dot_general(
                jnp.concatenate(left, axis=0), jnp.concatenate(right_of(c), axis=0), dims,
                preferred_element_type=jnp.float32) * scale

    @pl.when(pl.program_id(1) == 0)
    def _():
        write(lambda c: [r[c, :, :signals] for r in far] + [r[c, :, signals:] for r in far])

    @pl.when(pl.program_id(1) == 1)
    def _():
        write(lambda c: [-r[c, :, signals:] for r in far] + [r[c, :, :signals] for r in far])


def correlate(mine, far, place, scale, signals, partial=None):
    channels, peers, _ = mine[0].shape
    block = 16 if channels % 16 == 0 and peers <= 32 else 8
    spec = pl.BlockSpec((block, peers, 2 * signals), lambda i, h, p: (i, 0, 0))
    extra = [] if partial is None else [partial]
    count = 2 * len(mine)
    return pl.pallas_call(
        functools.partial(correlate_kernel, len(mine), signals, block, scale),
        grid_spec=pltpu.PrefetchScalarGridSpec(
            num_scalar_prefetch=1,
            grid=(channels // block, 2),
            in_specs=[spec] * count + [pl.BlockSpec(memory_space=pl.ANY)] * len(extra),
            out_specs=pl.BlockSpec(
                (block, signals, signals), lambda i, h, p: (i, 0, 2 * h + p[0])),
        ),
        out_shape=jax.ShapeDtypeStruct((channels, signals, 4 * signals), jnp.float32),
        input_output_aliases={1 + count: 0} if extra else {},
        compiler_params=pltpu.CompilerParams(
            dimension_semantics=("arbitrary", "arbitrary"), vmem_limit_bytes=40 * 1024 * 1024
        ),
        cost_estimate=pl.CostEstimate(
            flops=2_000_000_000, bytes_accessed=24_000_000, transcendentals=0
        ),
    )(place.astype(jnp.int32).reshape(1), *mine, *far, *extra)


def per_device(voltages, pfb_window):
    signals, samples = voltages.shape
    frames = samples // NFFT
    peers = lax.axis_size("ta")
    sides = lax.axis_size("aa")
    assert sides == 2 and frames >= TAPS - 1 and signals % LANES == 0
    onward = [(i, i + 1) for i in range(peers - 1)]
    across = [(i, 1 - i) for i in range(sides)]

    history = {}
    for frame in range(frames - 1, frames - TAPS, -1):
        tail = voltages[:, frame * NFFT : (frame + 1) * NFFT]
        history[frame - frames] = lax.ppermute(tail, "ta", onward)

    own, other, spectra = {}, {}, None

    def swap(frame, spectra_or_owned):
        owned = jnp.transpose(spectra_or_owned, (1, 0, 2))
        own[frame] = owned
        other[frame] = lax.ppermute(owned, "aa", across)

    turned = {}
    for frame in range(frames - 1, -1, -1):
        at_needed = frame - (TAPS - 1)
        if spectra is not None and at_needed < 0:
            held = (history[at_needed], spectra)
            if frame + 2 in turned:
                history[at_needed], _, turned[frame + 2] = lax.optimization_barrier(
                    held + (turned[frame + 2],))
            else:
                history[at_needed], _ = lax.optimization_barrier(held)
        if frame + 2 in turned:
            swap(frame + 2, turned.pop(frame + 2))
        pieces = []
        for tap in range(TAPS):
            at = frame - (TAPS - 1) + tap
            pieces.append((voltages, at) if at >= 0 else (history[at], 0))
        spectra = channelize(pieces, pfb_window, signals)
        if frame == 0:
            for late in sorted(turned, reverse=True):
                turned[late], spectra = lax.optimization_barrier((turned[late], spectra))
                swap(late, turned.pop(late))
        turned[frame] = lax.all_to_all(
            spectra.reshape(peers, CH // peers, 2 * signals), "ta",
            split_axis=0, concat_axis=0, tiled=True)
    for late in sorted(turned, reverse=True):
        swap(late, turned.pop(late))

    order = sorted(own)
    mine = [own[f] for f in order]
    scale = 1.0 / math.sqrt(frames * peers)
    side = lax.axis_index("aa")
    near = correlate(mine, mine, side, scale, signals)
    return correlate(mine, [other[f] for f in order], 1 - side, scale, signals, near)


def solution(mesh):
    in_specs = (P("aa", "ta"), P())
    out_specs = P("ta", "aa", None)
    return jax.shard_map(
        per_device, mesh=mesh, in_specs=in_specs, out_specs=out_specs, check_vma=False
    )
```

```python
import functools
import math

import jax
import jax.numpy as jnp
import numpy as np
from jax import lax
from jax.experimental import pallas as pl
from jax.experimental.pallas import tpu as pltpu
from jax.sharding import PartitionSpec as P


NFFT = 8192
CH = 2048
TAPS = 4
CH_OFF = 1024
RADIX = 32
INNER = NFFT // RADIX
BINS = CH // RADIX
HALF = RADIX // 2
LANES = 128
SIG_BLOCK = 16


def split_bf16(x):
    hi = jnp.asarray(x, jnp.bfloat16)
    return hi, (x - hi.astype(jnp.float32)).astype(jnp.bfloat16)


def stage_two_matrix():
    n2 = np.arange(INNER)[None, :]
    m = np.arange(BINS)[:, None] + CH_OFF // RADIX
    angle = 2.0 * np.pi * ((n2 * m) % INNER) / INNER
    mirror = 2.0 * np.pi * ((n2 * (m + 1)) % INNER) / INNER
    rows = [
        np.concatenate([np.cos(angle), np.sin(angle)], axis=1),
        np.concatenate([-np.sin(angle), np.cos(angle)], axis=1),
        np.concatenate([np.cos(mirror), -np.sin(mirror)], axis=1),
        np.concatenate([-np.sin(mirror), -np.cos(mirror)], axis=1),
    ]
    full = np.concatenate(rows, axis=0) / math.sqrt(NFFT)
    hi = full.astype(jnp.bfloat16)
    lo = (full - hi.astype(np.float64)).astype(jnp.bfloat16)
    return hi, lo


def twist_table():
    k = np.arange(HALF + 1)[:, None]
    n2 = np.arange(INNER)[None, :]
    angle = 2.0 * np.pi * (k * n2) / NFFT
    return np.stack([np.cos(angle), -np.sin(angle)]).astype(np.float32)


def rfft_list(x):
    n = len(x)
    if n == 2:
        return [(x[0] + x[1], None), (x[0] - x[1], None)]
    even, odd = rfft_list(x[0::2]), rfft_list(x[1::2])
    out = [None] * (n // 2 + 1)
    for k in range(n // 4 + 1):
        er, ei = even[k]
        our, oui = odd[k]
        if k == 0:
            out[0] = (er + our, None)
            out[n // 2] = (er - our, None)
        elif k == n // 4:
            out[k] = (er, -our)
        else:
            c = math.cos(2 * math.pi * k / n)
            s = math.sin(2 * math.pi * k / n)
            if 8 * k == n:
                tr, ti = (our + oui) * c, (oui - our) * c
            else:
                tr, ti = our * c + oui * s, oui * c - our * s
            out[k] = (er + tr, ei + ti)
            out[n // 2 - k] = (er - tr, ti - ei)
    return out


def channel_kernel(steps, signals, *refs):
    taps = refs[:TAPS]
    win, twist, mat_hi, mat_lo, out, parts_s, spec_s = refs[TAPS:]
    step = pl.program_id(0)
    rows = pl.ds(pl.multiple_of(step * SIG_BLOCK, SIG_BLOCK), SIG_BLOCK)
    low_rows = pl.ds(pl.multiple_of(signals + step * SIG_BLOCK, SIG_BLOCK), SIG_BLOCK)

    for part in range(INNER // LANES):
        filtered = []
        for n1 in range(RADIX):
            cols = pl.ds(n1 * INNER + part * LANES, LANES)
            total = win[0:1, cols] * taps[0][:, cols].astype(jnp.float32)
            for t in range(1, TAPS):
                total = total + win[t : t + 1, cols] * taps[t][:, cols].astype(jnp.float32)
            filtered.append(total)
        here = pl.ds(part * LANES, LANES)
        there = pl.ds(INNER + part * LANES, LANES)
        for k, (ar, ai) in enumerate(rfft_list(filtered)):
            if k == 0:
                br, bi = ar, jnp.zeros_like(ar)
            else:
                tr, ti = twist[0, k : k + 1, here], twist[1, k : k + 1, here]
                if ai is None:
                    br, bi = ar * tr, ar * ti
                else:
                    br, bi = ar * tr - ai * ti, ar * ti + ai * tr
            for value, cols in ((br, here), (bi, there)):
                hi, lo = split_bf16(value)
                parts_s[k, rows, cols] = hi
                parts_s[k, low_rows, cols] = lo

    @pl.when(step == steps - 1)
    def _():
        dims = (((1,), (1,)), ((), ()))

        def dot(a, b):
            return lax.dot_general(a, b, dims, preferred_element_type=jnp.float32)

        def put(value, k):
            spec_s[0, pl.ds(k, BINS, stride=RADIX), :] = value[:BINS]
            spec_s[1, pl.ds(k, BINS, stride=RADIX), :] = value[BINS:]

        for k in range(HALF + 1):
            size = 2 * BINS if k in (0, HALF) else 4 * BINS
            a_hi, a_lo = mat_hi[:size, :], mat_lo[:size, :]
            both = dot(a_hi, parts_s[k])
            small = dot(a_lo, parts_s[k, :signals])
            res = both[:, :signals] + (both[:, signals:] + small)
            put(res[: 2 * BINS], k)
            if size > 2 * BINS:
                put(res[2 * BINS :], RADIX - k)

        def cast(i, carry):
            at = pl.ds(pl.multiple_of(i * 64, 64), 64)
            out[at, :signals] = spec_s[0, at, :].astype(jnp.bfloat16)
            out[at, signals:] = spec_s[1, at, :].astype(jnp.bfloat16)
            return carry

        lax.fori_loop(0, CH // 64, cast, 0)


def channelize(pieces, window, signals):
    steps = signals // SIG_BLOCK
    mat_hi, mat_lo = stage_two_matrix()

    def tap_spec(frame):
        return pl.BlockSpec((SIG_BLOCK, NFFT), lambda i, frame=frame: (i, frame))

    whole = lambda shape: pl.BlockSpec(shape, lambda i: (0,) * len(shape))
    return pl.pallas_call(
        functools.partial(channel_kernel, steps, signals),
        grid=(steps,),
        out_shape=jax.ShapeDtypeStruct((CH, 2 * signals), jnp.bfloat16),
        in_specs=[tap_spec(frame) for _, frame in pieces]
        + [
            whole((TAPS, NFFT)),
            whole((2, HALF + 1, INNER)),
            whole((4 * BINS, 2 * INNER)),
            whole((4 * BINS, 2 * INNER)),
        ],
        out_specs=whole((CH, 2 * signals)),
        scratch_shapes=[
            pltpu.VMEM((HALF + 1, 2 * signals, 2 * INNER), jnp.bfloat16),
            pltpu.VMEM((2, CH, signals), jnp.float32),
        ],
        compiler_params=pltpu.CompilerParams(
            dimension_semantics=("arbitrary",), vmem_limit_bytes=48 * 1024 * 1024
        ),
        cost_estimate=pl.CostEstimate(
            flops=8_000_000_000, bytes_accessed=10_000_000, transcendentals=0
        ),
    )(
        *[piece for piece, _ in pieces],
        window,
        jnp.asarray(twist_table()),
        jnp.asarray(mat_hi),
        jnp.asarray(mat_lo),
    )


def correlate_kernel(chunks, signals, block, scale, *refs):
    mine = refs[1 : 1 + chunks]
    far = refs[1 + chunks : 1 + 2 * chunks]
    out = refs[-1]
    dims = (((0,), (0,)), ((), ()))

    def write(right_of):
        for c in range(block):
            left = [r[c, :, :signals] for r in mine] + [r[c, :, signals:] for r in mine]
            out[c] = lax.dot_general(
                jnp.concatenate(left, axis=0), jnp.concatenate(right_of(c), axis=0), dims,
                preferred_element_type=jnp.float32) * scale

    @pl.when(pl.program_id(1) == 0)
    def _():
        write(lambda c: [r[c, :, :signals] for r in far] + [r[c, :, signals:] for r in far])

    @pl.when(pl.program_id(1) == 1)
    def _():
        write(lambda c: [-r[c, :, signals:] for r in far] + [r[c, :, :signals] for r in far])


def correlate(mine, far, place, scale, signals, partial=None):
    channels, peers, _ = mine[0].shape
    block = 16 if channels % 16 == 0 and peers <= 32 else 8
    spec = pl.BlockSpec((block, peers, 2 * signals), lambda i, h, p: (i, 0, 0))
    extra = [] if partial is None else [partial]
    count = 2 * len(mine)
    return pl.pallas_call(
        functools.partial(correlate_kernel, len(mine), signals, block, scale),
        grid_spec=pltpu.PrefetchScalarGridSpec(
            num_scalar_prefetch=1,
            grid=(channels // block, 2),
            in_specs=[spec] * count + [pl.BlockSpec(memory_space=pl.ANY)] * len(extra),
            out_specs=pl.BlockSpec(
                (block, signals, signals), lambda i, h, p: (i, 0, 2 * h + p[0])),
        ),
        out_shape=jax.ShapeDtypeStruct((channels, signals, 4 * signals), jnp.float32),
        input_output_aliases={1 + count: 0} if extra else {},
        compiler_params=pltpu.CompilerParams(
            dimension_semantics=("arbitrary", "arbitrary"), vmem_limit_bytes=40 * 1024 * 1024
        ),
        cost_estimate=pl.CostEstimate(
            flops=2_000_000_000, bytes_accessed=24_000_000, transcendentals=0
        ),
    )(place.astype(jnp.int32).reshape(1), *mine, *far, *extra)


def per_device(voltages, pfb_window):
    signals, samples = voltages.shape
    frames = samples // NFFT
    peers = lax.axis_size("ta")
    sides = lax.axis_size("aa")
    assert sides == 2 and frames >= TAPS - 1 and signals % LANES == 0
    onward = [(i, i + 1) for i in range(peers - 1)]
    across = [(i, 1 - i) for i in range(sides)]

    history = {}
    for frame in range(frames - 1, frames - TAPS, -1):
        tail = voltages[:, frame * NFFT : (frame + 1) * NFFT]
        history[frame - frames] = lax.ppermute(tail, "ta", onward)

    def turn(spectra):
        return lax.all_to_all(
            spectra.reshape(peers, CH // peers, 2 * signals), "ta",
            split_axis=0, concat_axis=0, tiled=True)

    spectra, turned, own, other = {}, {}, {}, {}
    last = frames - 1
    for frame in range(last, -1, -1):
        oldest = frame - (TAPS - 1)
        if frame < last and oldest < 0:
            history[oldest], spectra[frame + 1] = lax.optimization_barrier(
                (history[oldest], spectra[frame + 1]))
        pieces = []
        for tap in range(TAPS):
            at = oldest + tap
            pieces.append((voltages, at) if at >= 0 else (history[at], 0))
        spectra[frame] = channelize(pieces, pfb_window, signals)
        if frame == last:
            turned[last] = turn(spectra[last])
    later = list(range(last - 1, -1, -1))
    held = lax.optimization_barrier([spectra[f] for f in later])
    for frame, value in zip(later, held):
        turned[frame] = turn(value)
    for frame in [last] + later:
        own[frame] = jnp.transpose(turned[frame], (1, 0, 2))
        other[frame] = lax.ppermute(own[frame], "aa", across)

    order = sorted(own)
    mine = [own[f] for f in order]
    scale = 1.0 / math.sqrt(frames * peers)
    side = lax.axis_index("aa")
    near = correlate(mine, mine, side, scale, signals)
    return correlate(mine, [other[f] for f in order], 1 - side, scale, signals, near)


def solution(mesh):
    in_specs = (P("aa", "ta"), P())
    out_specs = P("ta", "aa", None)
    return jax.shard_map(
        per_device, mesh=mesh, in_specs=in_specs, out_specs=out_specs, check_vma=False
    )
```
